32 devices in a mesh: gx: 8 (over z, x), gy: 4 (over y, core).
Axes of the slice: x: 2, y: 2, z: 4, core: 2. Of those that a mesh axis runs over, the one named last changes fastest.
Arguments:
- source_tiles: bfloat16 [96, 32, 192, 384], P(('gx', 'gy')), may hold values from -6 to 6
- tile_offsets: int32 [2, 96], P(None, ('gx', 'gy')), may hold values from -128 to 896, as said below
- tile_shifts: int32 [96], P(('gx', 'gy')), may hold values from 0 to 63
- tile_counts: int32 [32], P(('gx', 'gy')), may hold values from 1 to 3, as said below
Outputs:
- merged_slab: float32 [32, 1024, 1024], P(None, 'gx', 'gy')
The draws below stay inside these ranges and needn't reach their ends.
Inputs may be any that keep to these rules, and one draw needn't show every extreme that they name: `tile_offsets`: slot k belongs to the device of joined gx+gy index d = k // 3, that is gx index d // 4 and gy index d % 4. Its x offset lies from that gx index times 128 minus 64 up to that gx index times 128; its y offset from the gy index times 256 minus 128 up to the gy index times 256. So every tile covers its owner's whole block. `tile_counts`: entry d counts the used slots of device d; they are its first slots, the others are ignored. Both 1 and 3 occur in every draw.
All inputs are finite; a program needn't handle non-finite values.
Results may differ from the reference program's by a relative error of at most 0.0003.
Values sent between devices are 32-bit elements; how exact they have to be, the bound alone decides.
No kernel may reach another device: no remote copies, remote signals or barrier semaphores. Data moves between devices by JAX's collectives and lax.ppermute only.
A program may use at most 192 MiB of HBM per device.

```python
import jax
import jax.numpy as jnp
from jax import lax

NZ = 32
BX = 128
BY = 256
TX = 192
TY = 384
CAP = 3
RAMP = 32
NSHIFT = 64
RX = 64
RY = 128
NX = 1024
NY = 1024
TILES = 96


def draw_tile_offsets(key, part):
    holders = jnp.arange(TILES, dtype=jnp.int32) // CAP
    rows_gy = NY // BY
    column = holders // rows_gy
    row_place = holders % rows_gy
    key_x, key_y = jax.random.split(jax.random.fold_in(key, 11))
    back_x = jax.random.randint(key_x, (TILES,), 0, TX - BX + 1)
    back_y = jax.random.randint(key_y, (TILES,), 0, TY - BY + 1)
    back_x = back_x.at[0].set(TX - BX).at[TILES - 1].set(0)
    back_y = back_y.at[0].set(TY - BY).at[TILES - 1].set(0)
    return jnp.stack([column * BX - back_x, row_place * BY - back_y]).astype(jnp.int32)


def draw_tile_counts(key, part):
    counts = jax.random.randint(jax.random.fold_in(key, 23), (TILES // CAP,), 1, CAP + 1)
    counts = counts.at[0].set(CAP).at[1].set(1)
    return counts.astype(jnp.int32)


def plant(array, stream_key, smallest, top_value):
    longest = array.shape.index(max(array.shape))
    spots = []
    for shift in (0, 1):
        where = [jax.random.randint(jax.random.fold_in(stream_key, axis), (), 0, length) for axis, length in enumerate(array.shape)]
        where[longest] = (where[longest] + shift) % array.shape[longest]
        spots.append(tuple(where))
    return array.at[spots[0]].set(smallest).at[spots[1]].set(top_value)


def block_scale(rng, extent, shards, least, top_value):
    loudness = 1.0
    for dim, parts in shards:
        draws = jax.random.uniform(jax.random.fold_in(jax.random.fold_in(rng, 6), dim), (parts,), jnp.float32, least / len(shards), top_value / len(shards))
        loudness = loudness * jnp.repeat(jnp.exp(draws), extent[dim] // parts).reshape((-1,) + (1,) * (len(extent) - 1 - dim))
    return loudness


def noise(rng, extent, scale, bound, shards=(), kind=jnp.bfloat16):
    entries = scale * jax.random.normal(rng, extent, jnp.float32)
    if shards:
        entries = entries * block_scale(rng, extent, shards, -0.22, 0.18)
    return jnp.clip(entries, -bound, bound).astype(kind)


def setup_inputs(seed: int = 0) -> dict:
    streams_of = jax.random.split(jax.random.key(seed), 5)
    return {
        "source_tiles": noise(streams_of[0], (TILES, NZ, TX, TY), 1.0, 6.0, ((0, 32),)),
        "tile_offsets": draw_tile_offsets(jax.random.fold_in(streams_of[4], 71), 0),
        "tile_shifts": plant(jax.random.randint(streams_of[2], (TILES,), 0, NSHIFT), jax.random.fold_in(streams_of[2], 1), 0, NSHIFT - 1).astype(jnp.int32),
        "tile_counts": draw_tile_counts(jax.random.fold_in(streams_of[4], 71), 0),
    }


def interpolate(volume, fraction, dimension):
    length = volume.shape[dimension]
    shifted = jnp.concatenate([lax.slice_in_dim(volume, 1, length, axis=dimension), lax.slice_in_dim(volume, length - 1, length, axis=dimension)], axis=dimension)
    return (1.0 - fraction) * volume + fraction * shifted


def resample(source, shift_code):
    depth_part = ((shift_code // 16) % 4).astype(jnp.float32) * 0.25
    column_part = ((shift_code // 4) % 4).astype(jnp.float32) * 0.25
    row_part = (shift_code % 4).astype(jnp.float32) * 0.25
    volume = source.astype(jnp.float32)
    volume = interpolate(volume, depth_part, 0)
    volume = interpolate(volume, column_part, 1)
    return interpolate(volume, row_part, 2)


def blend_ramp(length):
    places = jnp.arange(length, dtype=jnp.float32)
    return jnp.minimum(jnp.minimum(places + 1.0, length - places), float(RAMP))


def reference(source_tiles, tile_offsets, tile_shifts, tile_counts):
    weight_plane = blend_ramp(TX)[:, None] * blend_ramp(TY)[None, :]
    values = jnp.zeros((NZ, NX + 2 * RX, NY + 2 * RY), jnp.float32)
    weights = jnp.zeros((NX + 2 * RX, NY + 2 * RY), jnp.float32)

    def place_tile(accumulated, number):
        values, weights = accumulated
        holder = number // CAP
        active = ((number % CAP) < tile_counts[holder]).astype(jnp.float32)
        source = lax.dynamic_index_in_dim(source_tiles, number, 0, keepdims=False)
        scaled = active * weight_plane
        volume = resample(source, tile_shifts[number]) * scaled[None]
        start_x = (tile_offsets[0, number] + RX).astype(jnp.int32)
        start_y = (tile_offsets[1, number] + RY).astype(jnp.int32)
        anchor = jnp.int32(0)
        window = lax.dynamic_slice(values, (anchor, start_x, start_y), (NZ, TX, TY))
        values = lax.dynamic_update_slice(values, window + volume, (anchor, start_x, start_y))
        weight_window = lax.dynamic_slice(weights, (start_x, start_y), (TX, TY))
        weights = lax.dynamic_update_slice(weights, weight_window + scaled, (start_x, start_y))
        return (values, weights), None

    (values, weights), ignored = lax.scan(place_tile, (values, weights), jnp.arange(TILES, dtype=jnp.int32))
    block_weights = weights[RX:RX + NX, RY:RY + NY]
    return values[:, RX:RX + NX, RY:RY + NY] / jnp.maximum(block_weights, 1.0)[None]
```

```python
import functools

import jax
import jax.numpy as jnp
from jax import lax
from jax.experimental import pallas as pl
from jax.experimental.pallas import tpu as pltpu
from jax.sharding import PartitionSpec as P

BX = 128
BY = 256
RAMP = 32
CHUNKS = 4
ZB = 4


def passed_along(array, axis, by):
    count = lax.axis_size(axis)
    pairs = [(i, i + by) for i in range(count) if 0 <= i + by < count]
    return lax.ppermute(array, axis, pairs)


def ramp_of(places, length):
    rise = jnp.minimum(jnp.minimum(places + 1, length - places), RAMP).astype(jnp.float32)
    return jnp.where((places >= 0) & (places < length), rise, 0.0)


def merge_kernel(params, src, nxt, low, mid, high, my, mx, acc, stack, *, cap, tx, ty, rx, ry):
    wide_x = BX + 2 * rx
    wide_y = BY + 2 * ry
    zb = src.shape[1]

    @pl.when(pl.program_id(0) == 0)
    def build():
        for k in range(cap):
            frac = (params[2 * cap + k] % 4).astype(jnp.float32) * 0.25
            place = lax.broadcasted_iota(jnp.int32, (1, wide_y), 1) - params[cap + k]
            ramp = ramp_of(place, ty)
            cell = lax.broadcasted_iota(jnp.int32, (ty, wide_y), 0)
            near = jnp.where(cell == place, ramp * (1.0 - frac), 0.0)
            far = jnp.where(cell == jnp.minimum(place + 1, ty - 1), ramp * frac, 0.0)
            my[k] = (near + far).astype(jnp.bfloat16)
        column = lax.broadcasted_iota(jnp.int32, (1, 2 * cap * tx), 1)
        column = jnp.where(column >= cap * tx, column - cap * tx, column)
        start = jnp.zeros_like(column)
        frac = jnp.zeros(column.shape, jnp.float32)
        active = jnp.zeros(column.shape, jnp.float32)
        cell = column
        for k in range(cap):
            here = (column >= k * tx) & (column < (k + 1) * tx)
            start = jnp.where(here, params[k], start)
            code = params[2 * cap + k] // 4 % 4
            frac = jnp.where(here, code.astype(jnp.float32) * 0.25, frac)
            active = jnp.where(here, params[3 * cap + k].astype(jnp.float32), active)
            cell = jnp.where(here, column - k * tx, cell)
        place = lax.broadcasted_iota(jnp.int32, (wide_x, 2 * cap * tx), 0) - start
        ramp = ramp_of(place, tx) * active
        near = jnp.where(cell == place, ramp * (1.0 - frac), 0.0)
        far = jnp.where(cell == jnp.minimum(place + 1, tx - 1), ramp * frac, 0.0)
        mx[...] = (near + far).astype(jnp.bfloat16)
        for k in range(cap):
            acc[k, zb * tx :] = jnp.dot(nxt[k, 0], my[k], preferred_element_type=jnp.float32)

    for k in range(cap):
        rows = src[k].reshape(zb * tx, ty)
        acc[k, : zb * tx] = jnp.dot(rows, my[k], preferred_element_type=jnp.float32)
    for j in range(zb):
        for k in range(cap):
            frac = (params[2 * cap + k] // 16 % 4).astype(jnp.float32) * 0.25
            here = acc[k, j * tx : (j + 1) * tx]
            after = acc[k, (j + 1) * tx : (j + 2) * tx]
            value = (1.0 - frac) * here + frac * after
            head = value.astype(jnp.bfloat16)
            stack[j % 2, k * tx : (k + 1) * tx] = head
            tail = (value - head.astype(jnp.float32)).astype(jnp.bfloat16)
            stack[j % 2, (cap + k) * tx : (cap + k + 1) * tx] = tail
        total = jnp.dot(mx[...], stack[j % 2], preferred_element_type=jnp.float32)
        low[j] = total[:, :ry]
        mid[j] = total[:, ry : ry + BY]
        high[j] = total[:, ry + BY :]
    for k in range(cap):
        acc[k, zb * tx :] = acc[k, :tx]


def merge_chunk(source, params, first, depth, rx, ry):
    cap, nz, tx, ty = source.shape
    steps = depth // ZB
    wide_x = BX + 2 * rx
    wide_y = BY + 2 * ry
    top = first // ZB + steps - 1
    after = min(first + depth, nz - 1)
    kernel = functools.partial(merge_kernel, cap=cap, tx=tx, ty=ty, rx=rx, ry=ry)
    return pl.pallas_call(
        kernel,
        grid=(steps,),
        in_specs=[
            pl.BlockSpec(memory_space=pltpu.SMEM),
            pl.BlockSpec((cap, ZB, tx, ty), lambda i: (0, top - i, 0, 0)),
            pl.BlockSpec((cap, 1, tx, ty), lambda i: (0, after, 0, 0)),
        ],
        out_specs=[
            pl.BlockSpec((ZB, wide_x, ry), lambda i: (steps - 1 - i, 0, 0)),
            pl.BlockSpec((ZB, wide_x, BY), lambda i: (steps - 1 - i, 0, 0)),
            pl.BlockSpec((ZB, wide_x, ry), lambda i: (steps - 1 - i, 0, 0)),
        ],
        out_shape=[
            jax.ShapeDtypeStruct((depth, wide_x, ry), jnp.float32),
            jax.ShapeDtypeStruct((depth, wide_x, BY), jnp.float32),
            jax.ShapeDtypeStruct((depth, wide_x, ry), jnp.float32),
        ],
        scratch_shapes=[
            pltpu.VMEM((cap, ty, wide_y), jnp.bfloat16),
            pltpu.VMEM((wide_x, 2 * cap * tx), jnp.bfloat16),
            pltpu.VMEM((cap, (ZB + 1) * tx, wide_y), jnp.float32),
            pltpu.VMEM((2, 2 * cap * tx, wide_y), jnp.bfloat16),
        ],
        compiler_params=pltpu.CompilerParams(
            dimension_semantics=("arbitrary",), vmem_limit_bytes=48 * 1024 * 1024
        ),
        cost_estimate=pl.CostEstimate(
            flops=depth * 2 * cap * tx * wide_y * (ty + 2 * wide_x),
            bytes_accessed=depth * (cap * tx * ty * 2 + wide_x * wide_y * 4),
            transcendentals=0,
        ),
        name="merge_tiles",
    )(params, source, source)


def rows_kernel(mid, before, after, low, high, *, rx, ry):
    edge = rx + BX
    low[:, :, :ry] = mid[:, :rx, :ry] + before[:, :rx]
    low[:, :, ry:] = mid[:, :rx, ry:] + after[:, :rx]
    high[:, :, :ry] = mid[:, edge:, :ry] + before[:, edge:]
    high[:, :, ry:] = mid[:, edge:, ry:] + after[:, edge:]


def edge_rows(mid, before, after, rx, ry):
    depth = mid.shape[0]
    step = min(depth, 4)
    whole = lambda a: pl.BlockSpec((step,) + a.shape[1:], lambda i: (i, 0, 0))
    shape = jax.ShapeDtypeStruct((depth, rx, BY), jnp.float32)
    return pl.pallas_call(
        functools.partial(rows_kernel, rx=rx, ry=ry),
        grid=(depth // step,),
        in_specs=[whole(mid), whole(before), whole(after)],
        out_specs=[whole(shape), whole(shape)],
        out_shape=[shape, shape],
        compiler_params=pltpu.CompilerParams(vmem_limit_bytes=48 * 1024 * 1024),
        cost_estimate=pl.CostEstimate(
            flops=depth * 2 * rx * BY, bytes_accessed=mid.size * 8, transcendentals=0
        ),
        name="edge_rows",
    )(mid, before, after)


def finish_kernel(mid, before, after, left, right, scale, *rest, rx, ry):
    out = rest[-1]
    low = slice(rx, 2 * rx)
    high = slice(2 * rx, 3 * rx)
    for rows, place, other in ((low, slice(0, rx), left), (high, slice(rx, 2 * rx), right)):
        part = mid[:, rows, :ry] + before[:, rows] + other[:, :, :ry]
        out[:, place, :ry] = part * scale[place, :ry]
        part = mid[:, rows, ry:] + after[:, rows] + other[:, :, ry:]
        out[:, place, ry:] = part * scale[place, ry:]


def finish_chunk(pieces, scale, out, first, nz, rx, ry):
    depth = pieces[0].shape[0]
    step = min(depth, 4)
    base = first // step
    whole = lambda a: pl.BlockSpec((step,) + a.shape[1:], lambda i: (i, 0, 0))
    specs = [whole(a) for a in pieces] + [pl.BlockSpec(scale.shape, lambda i: (0, 0))]
    operands = list(pieces) + [scale]
    aliases = {}
    if out is not None:
        aliases = {len(operands): 0}
        specs.append(pl.BlockSpec(memory_space=pl.ANY))
        operands.append(out)
    return pl.pallas_call(
        functools.partial(finish_kernel, rx=rx, ry=ry),
        grid=(depth // step,),
        in_specs=specs,
        out_specs=pl.BlockSpec((step, BX, BY), lambda i: (base + i, 0, 0)),
        out_shape=jax.ShapeDtypeStruct((nz, BX, BY), jnp.float32),
        input_output_aliases=aliases,
        compiler_params=pltpu.CompilerParams(vmem_limit_bytes=48 * 1024 * 1024),
        cost_estimate=pl.CostEstimate(
            flops=depth * 4 * BX * BY, bytes_accessed=pieces[0].size * 10, transcendentals=0
        ),
        name="finish_slab",
    )(*operands)


def weight_scale(own, tx, ty):
    band = jnp.concatenate([own, passed_along(own, "gy", 1), passed_along(own, "gy", -1)], axis=0)
    near = jnp.concatenate([band, passed_along(band, "gx", 1), passed_along(band, "gx", -1)], axis=0)
    cells_x = jnp.arange(BX, dtype=jnp.int32) + lax.axis_index("gx") * BX
    cells_y = jnp.arange(BY, dtype=jnp.int32) + lax.axis_index("gy") * BY
    ramp_x = ramp_of(cells_x[None] - near[:, 0:1], tx) * near[:, 2:3].astype(jnp.float32)
    ramp_y = ramp_of(cells_y[None] - near[:, 1:2], ty)
    weights = jnp.dot(ramp_x.T, ramp_y, precision=lax.Precision.HIGHEST)
    return 1.0 / jnp.maximum(weights, 1.0)


def local(source_tiles, tile_offsets, tile_shifts, tile_counts):
    cap, nz, tx, ty = source_tiles.shape
    rx = tx - BX
    ry = ty - BY
    active = (jnp.arange(cap, dtype=jnp.int32) < tile_counts[0]).astype(jnp.int32)
    starts_x = tile_offsets[0] - lax.axis_index("gx") * BX + rx
    starts_y = tile_offsets[1] - lax.axis_index("gy") * BY + ry
    params = jnp.concatenate([starts_x, starts_y, tile_shifts, active])
    scale = weight_scale(jnp.stack([tile_offsets[0], tile_offsets[1], active], axis=1), tx, ty)
    depth = nz // CHUNKS
    out = None
    waiting = []
    for number in range(CHUNKS):
        first = number * depth
        low, mid, high = merge_chunk(source_tiles, params, first, depth, rx, ry)
        after = passed_along(low, "gy", -1)
        before = passed_along(high, "gy", 1)
        edge_low, edge_high = edge_rows(mid, before, after, rx, ry)
        right = passed_along(edge_low, "gx", -1)
        left = passed_along(edge_high, "gx", 1)
        waiting.append((first, (mid, before, after, left, right)))
    for first, pieces in waiting:
        out = finish_chunk(pieces, scale, out, first, nz, rx, ry)
    return out


def solution(mesh):
    placed = (
        P(("gx", "gy"), None, None, None),
        P(None, ("gx", "gy")),
        P(("gx", "gy")),
        P(("gx", "gy")),
    )
    return jax.shard_map(
        local, mesh=mesh, in_specs=placed, out_specs=P(None, "gx", "gy"), check_vma=False
    )
```

```python
import functools

import jax
import jax.numpy as jnp
from jax import lax
from jax.experimental import pallas as pl
from jax.experimental.pallas import tpu as pltpu
from jax.sharding import PartitionSpec as P


BX = 128
BY = 256
RAMP = 32
CHUNKS = 4
ZB = 4


def passed_along(array, axis, by):
    count = lax.axis_size(axis)
    pairs = [(i, i + by) for i in range(count) if 0 <= i + by < count]
    return lax.ppermute(array, axis, pairs)


def ramp_of(places, length):
    rise = jnp.minimum(jnp.minimum(places + 1, length - places), RAMP).astype(jnp.float32)
    return jnp.where((places >= 0) & (places < length), rise, 0.0)


def merge_kernel(params, src, nxt, *rest, cap, tx, ty, rx, ry):
    low, mid, high, my, mx, acc, stack = rest[-7:]
    wide_x = BX + 2 * rx
    wide_y = BY + 2 * ry
    zb = src.shape[1]

    @pl.when(pl.program_id(0) == 0)
    def build():
        for k in range(cap):
            frac = (params[2 * cap + k] % 4).astype(jnp.float32) * 0.25
            place = lax.broadcasted_iota(jnp.int32, (1, wide_y), 1) - params[cap + k]
            ramp = ramp_of(place, ty)
            cell = lax.broadcasted_iota(jnp.int32, (ty, wide_y), 0)
            near = jnp.where(cell == place, ramp * (1.0 - frac), 0.0)
            far = jnp.where(cell == jnp.minimum(place + 1, ty - 1), ramp * frac, 0.0)
            my[k] = (near + far).astype(jnp.bfloat16)
        column = lax.broadcasted_iota(jnp.int32, (1, cap * tx), 1)
        start = jnp.zeros_like(column)
        frac = jnp.zeros(column.shape, jnp.float32)
        active = jnp.zeros(column.shape, jnp.float32)
        cell = column
        for k in range(cap):
            here = (column >= k * tx) & (column < (k + 1) * tx)
            start = jnp.where(here, params[k], start)
            code = params[2 * cap + k] // 4 % 4
            frac = jnp.where(here, code.astype(jnp.float32) * 0.25, frac)
            active = jnp.where(here, params[3 * cap + k].astype(jnp.float32), active)
            cell = jnp.where(here, column - k * tx, cell)
        place = lax.broadcasted_iota(jnp.int32, (wide_x, cap * tx), 0) - start
        ramp = ramp_of(place, tx) * active
        near = jnp.where(cell == place, ramp * (1.0 - frac), 0.0)
        far = jnp.where(cell == jnp.minimum(place + 1, tx - 1), ramp * frac, 0.0)
        both = (near + far).astype(jnp.bfloat16)
        mx[...] = jnp.concatenate([both, both], axis=1)
        for k in range(cap):
            acc[k, zb * tx :] = jnp.dot(nxt[k, 0], my[k], preferred_element_type=jnp.float32)

    for k in range(cap):
        rows = src[k].reshape(zb * tx, ty)
        half = wide_y // 2
        skip = half - ry
        acc[k, : zb * tx, :half] = jnp.dot(
            rows, my[k, :, :half], preferred_element_type=jnp.float32
        )
        acc[k, : zb * tx, half:] = jnp.dot(
            rows[:, skip:], my[k, skip:, half:], preferred_element_type=jnp.float32
        )
    for j in range(zb):
        for k in range(cap):
            frac = (params[2 * cap + k] // 16 % 4).astype(jnp.float32) * 0.25
            here = acc[k, j * tx : (j + 1) * tx]
            after = acc[k, (j + 1) * tx : (j + 2) * tx]
            value = (1.0 - frac) * here + frac * after
            head = value.astype(jnp.bfloat16)
            stack[j % 2, k * tx : (k + 1) * tx] = head
            tail = (value - head.astype(jnp.float32)).astype(jnp.bfloat16)
            stack[j % 2, (cap + k) * tx : (cap + k + 1) * tx] = tail
        total = jnp.dot(mx[...], stack[j % 2], preferred_element_type=jnp.float32)
        low[j] = total[:, :ry]
        mid[j] = total[:, ry : ry + BY]
        high[j] = total[:, ry + BY :]
    for k in range(cap):
        acc[k, zb * tx :] = acc[k, :tx]


def merge_chunk(source, params, first, depth, rx, ry, behind):
    cap, nz, tx, ty = source.shape
    steps = depth // ZB
    wide_x = BX + 2 * rx
    wide_y = BY + 2 * ry
    top = first // ZB + steps - 1
    after = min(first + depth, nz - 1)
    kernel = functools.partial(merge_kernel, cap=cap, tx=tx, ty=ty, rx=rx, ry=ry)
    return pl.pallas_call(
        kernel,
        grid=(steps,),
        in_specs=[
            pl.BlockSpec(memory_space=pltpu.SMEM),
            pl.BlockSpec((cap, ZB, tx, ty), lambda i: (0, top - i, 0, 0)),
            pl.BlockSpec((cap, 1, tx, ty), lambda i: (0, after, 0, 0)),
        ]
        + [pl.BlockSpec(memory_space=pl.ANY)] * len(behind),
        out_specs=[
            pl.BlockSpec((ZB, wide_x, ry), lambda i: (steps - 1 - i, 0, 0)),
            pl.BlockSpec((ZB, wide_x, BY), lambda i: (steps - 1 - i, 0, 0)),
            pl.BlockSpec((ZB, wide_x, ry), lambda i: (steps - 1 - i, 0, 0)),
        ],
        out_shape=[
            jax.ShapeDtypeStruct((depth, wide_x, ry), jnp.float32),
            jax.ShapeDtypeStruct((depth, wide_x, BY), jnp.float32),
            jax.ShapeDtypeStruct((depth, wide_x, ry), jnp.float32),
        ],
        scratch_shapes=[
            pltpu.VMEM((cap, ty, wide_y), jnp.bfloat16),
            pltpu.VMEM((wide_x, 2 * cap * tx), jnp.bfloat16),
            pltpu.VMEM((cap, (ZB + 1) * tx, wide_y), jnp.float32),
            pltpu.VMEM((2, 2 * cap * tx, wide_y), jnp.bfloat16),
        ],
        compiler_params=pltpu.CompilerParams(
            dimension_semantics=("arbitrary",), vmem_limit_bytes=48 * 1024 * 1024
        ),
        cost_estimate=pl.CostEstimate(
            flops=depth * 2 * cap * tx * wide_y * (ty + 2 * wide_x),
            bytes_accessed=depth * (cap * tx * ty * 2 + wide_x * wide_y * 4),
            transcendentals=0,
        ),
        name="merge_tiles",
    )(params, source, source, *behind)


def rows_kernel(mid, before, after, low, high, *, rx, ry):
    edge = rx + BX
    low[:, :, :ry] = mid[:, :rx, :ry] + before[:, :rx]
    low[:, :, ry:] = mid[:, :rx, ry:] + after[:, :rx]
    high[:, :, :ry] = mid[:, edge:, :ry] + before[:, edge:]
    high[:, :, ry:] = mid[:, edge:, ry:] + after[:, edge:]


def edge_rows(mid, before, after, rx, ry):
    depth = mid.shape[0]
    step = min(depth, 4)
    whole = lambda a: pl.BlockSpec((step,) + a.shape[1:], lambda i: (i, 0, 0))
    shape = jax.ShapeDtypeStruct((depth, rx, BY), jnp.float32)
    return pl.pallas_call(
        functools.partial(rows_kernel, rx=rx, ry=ry),
        grid=(depth // step,),
        in_specs=[whole(mid), whole(before), whole(after)],
        out_specs=[whole(shape), whole(shape)],
        out_shape=[shape, shape],
        compiler_params=pltpu.CompilerParams(vmem_limit_bytes=48 * 1024 * 1024),
        cost_estimate=pl.CostEstimate(
            flops=depth * 2 * rx * BY, bytes_accessed=mid.size * 8, transcendentals=0
        ),
        name="edge_rows",
    )(mid, before, after)


def finish_kernel(mid, before, after, left, right, scale, *rest, rx, ry):
    out = rest[-1]
    low = slice(rx, 2 * rx)
    high = slice(2 * rx, 3 * rx)
    for rows, place, other in ((low, slice(0, rx), left), (high, slice(rx, 2 * rx), right)):
        part = mid[:, rows, :ry] + before[:, rows] + other[:, :, :ry]
        out[:, place, :ry] = part * scale[place, :ry]
        part = mid[:, rows, ry:] + after[:, rows] + other[:, :, ry:]
        out[:, place, ry:] = part * scale[place, ry:]


def finish_chunk(pieces, scale, out, first, nz, rx, ry):
    depth = pieces[0].shape[0]
    step = min(depth, 4)
    base = first // step
    whole = lambda a: pl.BlockSpec((step,) + a.shape[1:], lambda i: (i, 0, 0))
    specs = [whole(a) for a in pieces] + [pl.BlockSpec(scale.shape, lambda i: (0, 0))]
    operands = list(pieces) + [scale]
    aliases = {}
    if out is not None:
        aliases = {len(operands): 0}
        specs.append(pl.BlockSpec(memory_space=pl.ANY))
        operands.append(out)
    return pl.pallas_call(
        functools.partial(finish_kernel, rx=rx, ry=ry),
        grid=(depth // step,),
        in_specs=specs,
        out_specs=pl.BlockSpec((step, BX, BY), lambda i: (base + i, 0, 0)),
        out_shape=jax.ShapeDtypeStruct((nz, BX, BY), jnp.float32),
        input_output_aliases=aliases,
        compiler_params=pltpu.CompilerParams(vmem_limit_bytes=48 * 1024 * 1024),
        cost_estimate=pl.CostEstimate(
            flops=depth * 4 * BX * BY, bytes_accessed=pieces[0].size * 10, transcendentals=0
        ),
        name="finish_slab",
    )(*operands)


def weight_scale(own, tx, ty):
    band = jnp.concatenate([own, passed_along(own, "gy", 1), passed_along(own, "gy", -1)], axis=0)
    from_left = passed_along(band, "gx", 1)
    from_right = passed_along(band, "gx", -1)
    near = jnp.concatenate([band, from_left, from_right], axis=0)
    cells_x = jnp.arange(BX, dtype=jnp.int32) + lax.axis_index("gx") * BX
    cells_y = jnp.arange(BY, dtype=jnp.int32) + lax.axis_index("gy") * BY
    ramp_x = ramp_of(cells_x[None] - near[:, 0:1], tx) * near[:, 2:3].astype(jnp.float32)
    ramp_y = ramp_of(cells_y[None] - near[:, 1:2], ty)
    weights = jnp.dot(ramp_x.T, ramp_y, precision=lax.Precision.HIGHEST)
    return 1.0 / jnp.maximum(weights, 1.0)


def merged(source_tiles, tile_offsets, tile_shifts, tile_counts):
    cap, nz, tx, ty = source_tiles.shape
    rx = tx - BX
    ry = ty - BY
    active = (jnp.arange(cap, dtype=jnp.int32) < tile_counts[0]).astype(jnp.int32)
    starts_x = tile_offsets[0] - lax.axis_index("gx") * BX + rx
    starts_y = tile_offsets[1] - lax.axis_index("gy") * BY + ry
    params = jnp.concatenate([starts_x, starts_y, tile_shifts, active])
    scale = weight_scale(jnp.stack([tile_offsets[0], tile_offsets[1], active], axis=1), tx, ty)
    depth = nz // CHUNKS
    out = None
    waiting = []
    edges = []
    for number in range(CHUNKS):
        first = number * depth
        behind = edges[number - 2] if number >= 2 else []
        low, mid, high = merge_chunk(source_tiles, params, first, depth, rx, ry, behind)
        after = passed_along(low, "gy", -1)
        before = passed_along(high, "gy", 1)
        edge_low, edge_high = edge_rows(mid, before, after, rx, ry)
        edges.append([edge_low])
        right = passed_along(edge_low, "gx", -1)
        left = passed_along(edge_high, "gx", 1)
        waiting.append((first, (mid, before, after, left, right)))
    for first, pieces in waiting:
        out = finish_chunk(pieces, scale, out, first, nz, rx, ry)
    return out


def solution(mesh):
    placed = (
        P(("gx", "gy"), None, None, None),
        P(None, ("gx", "gy")),
        P(("gx", "gy")),
        P(("gx", "gy")),
    )
    return jax.shard_map(
        merged, mesh=mesh, in_specs=placed, out_specs=P(None, "gx", "gy"), check_vma=False
    )
```

```python
import functools

import jax
import jax.numpy as jnp
from jax import lax
from jax.experimental import pallas as pl
from jax.experimental.pallas import tpu as pltpu
from jax.sharding import PartitionSpec as P


BX = 128
BY = 256
RAMP = 32
CHUNKS = 4
ZB = 2


def passed_along(array, axis, by):
    count = lax.axis_size(axis)
    pairs = [(i, i + by) for i in range(count) if 0 <= i + by < count]
    return lax.ppermute(array, axis, pairs)


def ramp_of(places, length):
    rise = jnp.minimum(jnp.minimum(places + 1, length - places), RAMP).astype(jnp.float32)
    return jnp.where((places >= 0) & (places < length), rise, 0.0)


def merge_kernel(params, src, nxt, *rest, cap, tx, ty, rx, ry):
    low, mid, high, my, mx, acc, stack = rest[-7:]
    wide_x = BX + 2 * rx
    wide_y = BY + 2 * ry
    zb = src.shape[1]

    @pl.when(pl.program_id(0) == 0)
    def build():
        for k in range(cap):
            frac = (params[2 * cap + k] % 4).astype(jnp.float32) * 0.25
            place = lax.broadcasted_iota(jnp.int32, (1, wide_y), 1) - params[cap + k]
            ramp = ramp_of(place, ty)
            cell = lax.broadcasted_iota(jnp.int32, (ty, wide_y), 0)
            near = jnp.where(cell == place, ramp * (1.0 - frac), 0.0)
            far = jnp.where(cell == jnp.minimum(place + 1, ty - 1), ramp * frac, 0.0)
            my[k] = (near + far).astype(jnp.bfloat16)
        column = lax.broadcasted_iota(jnp.int32, (1, cap * tx), 1)
        start = jnp.zeros_like(column)
        frac = jnp.zeros(column.shape, jnp.float32)
        active = jnp.zeros(column.shape, jnp.float32)
        cell = column
        for k in range(cap):
            here = (column >= k * tx) & (column < (k + 1) * tx)
            start = jnp.where(here, params[k], start)
            code = params[2 * cap + k] // 4 % 4
            frac = jnp.where(here, code.astype(jnp.float32) * 0.25, frac)
            active = jnp.where(here, params[3 * cap + k].astype(jnp.float32), active)
            cell = jnp.where(here, column - k * tx, cell)
        place = lax.broadcasted_iota(jnp.int32, (wide_x, cap * tx), 0) - start
        ramp = ramp_of(place, tx) * active
        near = jnp.where(cell == place, ramp * (1.0 - frac), 0.0)
        far = jnp.where(cell == jnp.minimum(place + 1, tx - 1), ramp * frac, 0.0)
        both = (near + far).astype(jnp.bfloat16)
        mx[...] = jnp.concatenate([both, both], axis=1)
        for k in range(cap):
            acc[k, zb * tx :] = jnp.dot(nxt[k, 0], my[k], preferred_element_type=jnp.float32)

    for k in range(cap):
        rows = src[k].reshape(zb * tx, ty)
        half = wide_y // 2
        skip = half - ry
        acc[k, : zb * tx, :half] = jnp.dot(
            rows, my[k, :, :half], preferred_element_type=jnp.float32
        )
        acc[k, : zb * tx, half:] = jnp.dot(
            rows[:, skip:], my[k, skip:, half:], preferred_element_type=jnp.float32
        )
    for j in range(zb):
        for k in range(cap):
            frac = (params[2 * cap + k] // 16 % 4).astype(jnp.float32) * 0.25
            here = acc[k, j * tx : (j + 1) * tx]
            after = acc[k, (j + 1) * tx : (j + 2) * tx]
            value = (1.0 - frac) * here + frac * after
            head = value.astype(jnp.bfloat16)
            stack[j % 2, k * tx : (k + 1) * tx] = head
            tail = (value - head.astype(jnp.float32)).astype(jnp.bfloat16)
            stack[j % 2, (cap + k) * tx : (cap + k + 1) * tx] = tail
        total = jnp.dot(mx[...], stack[j % 2], preferred_element_type=jnp.float32)
        low[j] = total[:, :ry]
        mid[j] = total[:, ry : ry + BY]
        high[j] = total[:, ry + BY :]
    for k in range(cap):
        acc[k, zb * tx :] = acc[k, :tx]


def merge_chunk(source, params, first, depth, rx, ry, behind):
    cap, nz, tx, ty = source.shape
    steps = depth // ZB
    wide_x = BX + 2 * rx
    wide_y = BY + 2 * ry
    top = first // ZB + steps - 1
    after = min(first + depth, nz - 1)
    kernel = functools.partial(merge_kernel, cap=cap, tx=tx, ty=ty, rx=rx, ry=ry)
    return pl.pallas_call(
        kernel,
        grid=(steps,),
        in_specs=[
            pl.BlockSpec(memory_space=pltpu.SMEM),
            pl.BlockSpec((cap, ZB, tx, ty), lambda i: (0, top - i, 0, 0)),
            pl.BlockSpec((cap, 1, tx, ty), lambda i: (0, after, 0, 0)),
        ]
        + [pl.BlockSpec(memory_space=pl.ANY)] * len(behind),
        out_specs=[
            pl.BlockSpec((ZB, wide_x, ry), lambda i: (steps - 1 - i, 0, 0)),
            pl.BlockSpec((ZB, wide_x, BY), lambda i: (steps - 1 - i, 0, 0)),
            pl.BlockSpec((ZB, wide_x, ry), lambda i: (steps - 1 - i, 0, 0)),
        ],
        out_shape=[
            jax.ShapeDtypeStruct((depth, wide_x, ry), jnp.float32),
            jax.ShapeDtypeStruct((depth, wide_x, BY), jnp.float32),
            jax.ShapeDtypeStruct((depth, wide_x, ry), jnp.float32),
        ],
        scratch_shapes=[
            pltpu.VMEM((cap, ty, wide_y), jnp.bfloat16),
            pltpu.VMEM((wide_x, 2 * cap * tx), jnp.bfloat16),
            pltpu.VMEM((cap, (ZB + 1) * tx, wide_y), jnp.float32),
            pltpu.VMEM((2, 2 * cap * tx, wide_y), jnp.bfloat16),
        ],
        compiler_params=pltpu.CompilerParams(
            dimension_semantics=("arbitrary",), vmem_limit_bytes=48 * 1024 * 1024
        ),
        cost_estimate=pl.CostEstimate(
            flops=depth * 2 * cap * tx * wide_y * (ty + 2 * wide_x),
            bytes_accessed=depth * (cap * tx * ty * 2 + wide_x * wide_y * 4),
            transcendentals=0,
        ),
        name="merge_tiles",
    )(params, source, source, *behind)


def rows_kernel(mid, before, after, low, high, *, rx, ry):
    edge = rx + BX
    low[:, :, :ry] = mid[:, :rx, :ry] + before[:, :rx]
    low[:, :, ry:] = mid[:, :rx, ry:] + after[:, :rx]
    high[:, :, :ry] = mid[:, edge:, :ry] + before[:, edge:]
    high[:, :, ry:] = mid[:, edge:, ry:] + after[:, edge:]


def edge_rows(mid, before, after, rx, ry):
    depth = mid.shape[0]
    step = 2
    whole = lambda a: pl.BlockSpec((step,) + a.shape[1:], lambda i: (i, 0, 0))
    shape = jax.ShapeDtypeStruct((depth, rx, BY), jnp.float32)
    return pl.pallas_call(
        functools.partial(rows_kernel, rx=rx, ry=ry),
        grid=(depth // step,),
        in_specs=[whole(mid), whole(before), whole(after)],
        out_specs=[whole(shape), whole(shape)],
        out_shape=[shape, shape],
        compiler_params=pltpu.CompilerParams(vmem_limit_bytes=48 * 1024 * 1024),
        cost_estimate=pl.CostEstimate(
            flops=depth * 2 * rx * BY, bytes_accessed=mid.size * 8, transcendentals=0
        ),
        name="edge_rows",
    )(mid, before, after)


def finish_kernel(mid, before, after, left, right, scale, *rest, rx, ry):
    out = rest[-1]
    low = slice(rx, 2 * rx)
    high = slice(2 * rx, 3 * rx)
    for rows, place, other in ((low, slice(0, rx), left), (high, slice(rx, 2 * rx), right)):
        part = mid[:, rows, :ry] + before[:, rows] + other[:, :, :ry]
        out[:, place, :ry] = part * scale[place, :ry]
        part = mid[:, rows, ry:] + after[:, rows] + other[:, :, ry:]
        out[:, place, ry:] = part * scale[place, ry:]


def finish_chunk(pieces, scale, out, first, nz, rx, ry):
    depth = pieces[0].shape[0]
    step = 2
    base = first // step
    whole = lambda a: pl.BlockSpec((step,) + a.shape[1:], lambda i: (i, 0, 0))
    specs = [whole(a) for a in pieces] + [pl.BlockSpec(scale.shape, lambda i: (0, 0))]
    operands = list(pieces) + [scale]
    aliases = {}
    if out is not None:
        aliases = {len(operands): 0}
        specs.append(pl.BlockSpec(memory_space=pl.ANY))
        operands.append(out)
    return pl.pallas_call(
        functools.partial(finish_kernel, rx=rx, ry=ry),
        grid=(depth // step,),
        in_specs=specs,
        out_specs=pl.BlockSpec((step, BX, BY), lambda i: (base + i, 0, 0)),
        out_shape=jax.ShapeDtypeStruct((nz, BX, BY), jnp.float32),
        input_output_aliases=aliases,
        compiler_params=pltpu.CompilerParams(vmem_limit_bytes=48 * 1024 * 1024),
        cost_estimate=pl.CostEstimate(
            flops=depth * 4 * BX * BY, bytes_accessed=pieces[0].size * 10, transcendentals=0
        ),
        name="finish_slab",
    )(*operands)


def weight_scale(own, tx, ty):
    band = jnp.concatenate([own, passed_along(own, "gy", 1), passed_along(own, "gy", -1)], axis=0)
    from_left = passed_along(band, "gx", 1)
    from_right = passed_along(band, "gx", -1)
    near = jnp.concatenate([band, from_left, from_right], axis=0)
    cells_x = jnp.arange(BX, dtype=jnp.int32) + lax.axis_index("gx") * BX
    cells_y = jnp.arange(BY, dtype=jnp.int32) + lax.axis_index("gy") * BY
    ramp_x = ramp_of(cells_x[None] - near[:, 0:1], tx) * near[:, 2:3].astype(jnp.float32)
    ramp_y = ramp_of(cells_y[None] - near[:, 1:2], ty)
    weights = jnp.dot(ramp_x.T, ramp_y, precision=lax.Precision.HIGHEST)
    return 1.0 / jnp.maximum(weights, 1.0)


def merged(source_tiles, tile_offsets, tile_shifts, tile_counts):
    cap, nz, tx, ty = source_tiles.shape
    rx = tx - BX
    ry = ty - BY
    active = (jnp.arange(cap, dtype=jnp.int32) < tile_counts[0]).astype(jnp.int32)
    starts_x = tile_offsets[0] - lax.axis_index("gx") * BX + rx
    starts_y = tile_offsets[1] - lax.axis_index("gy") * BY + ry
    params = jnp.concatenate([starts_x, starts_y, tile_shifts, active])
    scale = weight_scale(jnp.stack([tile_offsets[0], tile_offsets[1], active], axis=1), tx, ty)
    shift = nz // (4 * CHUNKS)
    depths = [nz // CHUNKS] * CHUNKS
    depths[0] -= shift
    depths[-1] += shift
    out = None
    waiting = []
    edges = []
    for number in range(CHUNKS):
        depth = depths[number]
        first = sum(depths[:number])
        behind = edges[number - 2] if number >= 2 else []
        low, mid, high = merge_chunk(source_tiles, params, first, depth, rx, ry, behind)
        after = passed_along(low, "gy", -1)
        before = passed_along(high, "gy", 1)
        edge_low, edge_high = edge_rows(mid, before, after, rx, ry)
        edges.append([edge_low])
        right = passed_along(edge_low, "gx", -1)
        left = passed_along(edge_high, "gx", 1)
        waiting.append((first, (mid, before, after, left, right)))
    for first, pieces in waiting:
        out = finish_chunk(pieces, scale, out, first, nz, rx, ry)
    return out


def solution(mesh):
    placed = (
        P(("gx", "gy"), None, None, None),
        P(None, ("gx", "gy")),
        P(("gx", "gy")),
        P(("gx", "gy")),
    )
    return jax.shard_map(
        merged, mesh=mesh, in_specs=placed, out_specs=P(None, "gx", "gy"), check_vma=False
    )
```
